512 devices in a mesh: wide: 128 (over z, y, core), quad: 4 (over x).
Axes of the slice: x: 4, y: 8, z: 8, core: 2. Of those that a mesh axis runs over, the one named last changes fastest.
Arguments:
- orbitals: float32 [256, 64, 4096], P('wide', 'quad'), may hold values from -6 to 6
- corners: int32 [256, 2], P('wide'), may hold values from 0 to 16
- pair_partner: int32 [512], P('wide'), may hold values from 0 to 255, as said below
- pair_live: int32 [512], P('wide'), may hold values from 0 to 1, as said below
Outputs:
- exchange_action: float32 [256, 64, 4096], P('wide', 'quad')
The draws below stay inside these ranges and needn't reach their ends.
Inputs may be any that keep to these rules, and one draw needn't show every extreme that they name: For the slots of owner w, the second orbital lies between the first plus 1 and the first plus 4 where the slot is live; every pair_partner is a valid orbital index. The number of live slots differs from owner to owner, and owner 0 has all 4 live. `pair_live`: dead slots may stand anywhere among an owner's slots.
All inputs are finite; a program needn't handle non-finite values.
Results may differ from the reference program's by a relative error of at most 0.0003.
Values sent between devices are 32-bit elements; how exact they have to be, the bound alone decides.
No kernel may reach another device: no remote copies, remote signals or barrier semaphores. Data moves between devices by JAX's collectives and lax.ppermute only.
A program may use at most 64 MiB of HBM per device.

```python
import math
import jax
import jax.numpy as jnp
from jax import lax

BX = 64
BY = 64
BZ = 64
SPAN = 16
ORB_DEV = 2
PAIR_DEV = 4
SWEEPS = 8
REACH = 4
ORB = 256
PAIRS = 512


def pair_tables(key):
    slots = jnp.arange(PAIRS, dtype=jnp.int32)
    owner = slots // PAIR_DEV
    within = slots % PAIR_DEV
    first = owner * ORB_DEV + within % ORB_DEV
    delta = jax.random.randint(jax.random.fold_in(key, 7), (PAIRS,), 1, REACH + 1)
    counts = jax.random.randint(jax.random.fold_in(key, 8), (PAIRS // PAIR_DEV,), 2, PAIR_DEV + 1)
    counts = counts.at[0].set(PAIR_DEV)
    second = first + delta
    live = (within < counts[owner]) & (second < ORB)
    second = jnp.minimum(second, ORB - 1)
    return (second.astype(jnp.int32), live.astype(jnp.int32))


def draw_pair_partner(key, part):
    return pair_tables(key)[0]


def draw_pair_live(key, part):
    return pair_tables(key)[1]


def set_ends(values, own_key, smallest, top_value):
    place = [jax.random.randint(jax.random.fold_in(own_key, axis), (), 0, length) for axis, length in enumerate(values.shape)]
    main_axis = values.shape.index(max(values.shape))
    next_to = place[:main_axis] + [(place[main_axis] + 1) % values.shape[main_axis]] + place[main_axis + 1:]
    return values.at[tuple(place)].set(smallest).at[tuple(next_to)].set(top_value)


def shard_levels(rng, extent, cuts, low, high):
    def one(dim, parts):
        heights = jax.random.uniform(jax.random.fold_in(jax.random.fold_in(rng, 6), dim), (parts,), jnp.float32, low / len(cuts), high / len(cuts))
        return jnp.repeat(jnp.exp(heights), extent[dim] // parts).reshape((-1,) + (1,) * (len(extent) - dim - 1))

    level = one(*cuts[0])
    for cut in cuts[1:]:
        level = level * one(*cut)
    return level


def normal_values(rng, dims, spread, most, shards=(), kind=jnp.bfloat16):
    gain = shard_levels(rng, dims, shards, -0.22, 0.18) if shards else 1.0
    values = jax.random.normal(rng, dims, jnp.float32) * spread * gain
    return jnp.minimum(jnp.maximum(values, -most), most).astype(kind)


def setup_inputs(seed: int = 0) -> dict:
    key_of = jax.random.split(jax.random.key(seed), 5)
    return {
        "orbitals": normal_values(key_of[0], (ORB, BX, BY * BZ), 1.0, 6.0, ((0, 128), (1, 4)), jnp.float32),
        "corners": set_ends(jax.random.randint(key_of[1], (ORB, 2), 0, SPAN + 1), jax.random.fold_in(key_of[1], 1), 0, SPAN).astype(jnp.int32),
        "pair_partner": draw_pair_partner(jax.random.fold_in(key_of[4], 71), 0),
        "pair_live": draw_pair_live(jax.random.fold_in(key_of[4], 71), 0),
    }


def sweep_weights():
    low = 0.5 / 6.5
    high = 12.5 / 6.5
    center = (high + low) / 2.0
    half = (high - low) / 2.0
    return [1.0 / (center + half * math.cos(math.pi * (2 * k + 1) / (2 * SWEEPS))) for k in range(SWEEPS)]


def move_box(box, shift_y, shift_z):
    margin = SPAN * BZ + SPAN
    flat = box.shape[-1]
    padded = jnp.pad(box, ((0, 0), (margin, margin)))
    start = (margin - shift_y * BZ - shift_z).astype(jnp.int32)
    taken = lax.dynamic_slice_in_dim(padded, start, flat, 1)
    source = jnp.arange(flat, dtype=jnp.int32) % BZ - shift_z
    keep = (source >= 0) & (source < BZ)
    return jnp.where(keep[None, :], taken, jnp.zeros_like(taken))


def neighbours(field, padded):
    flat = field.shape[-1]
    zpos = jnp.arange(flat, dtype=jnp.int32) % BZ
    total = padded[:, 2:] + padded[:, :-2]
    upper_z = jnp.pad(field[..., 1:], ((0, 0), (0, 0), (0, 1)))
    lower_z = jnp.pad(field[..., :-1], ((0, 0), (0, 0), (1, 0)))
    total = total + jnp.where(zpos < BZ - 1, upper_z, 0.0) + jnp.where(zpos > 0, lower_z, 0.0)
    total = total + jnp.pad(field[..., BZ:], ((0, 0), (0, 0), (0, BZ)))
    total = total + jnp.pad(field[..., :-BZ], ((0, 0), (0, 0), (BZ, 0)))
    return total


def solve_local(density):
    weights = sweep_weights()
    potential = weights[0] * density / 6.5
    for k in range(1, SWEEPS):
        padded = jnp.pad(potential, ((0, 0), (1, 1), (0, 0)))
        applied = 6.5 * potential - neighbours(potential, padded)
        potential = potential + weights[k] * (density - applied) / 6.5
    return potential


def reference(orbitals, corners, pair_partner, pair_live):
    slots = jnp.arange(PAIRS, dtype=jnp.int32)
    first = (slots // PAIR_DEV) * ORB_DEV + (slots % PAIR_DEV) % ORB_DEV

    def one_pair(total, item):
        left, right, live = item
        own = orbitals[left]
        offset = corners[right] - corners[left]
        moved = move_box(orbitals[right], offset[0], offset[1])
        density = own * moved * live.astype(jnp.float32)
        potential = solve_local(density[None])[0]
        total = total.at[left].add(potential * moved)
        total = total.at[right].add(move_box(potential * own, -offset[0], -offset[1]))
        return total, None

    start = jnp.zeros(orbitals.shape, jnp.float32)
    result, unused = lax.scan(one_pair, start, (first, pair_partner, pair_live))
    return result
```

```python
import functools
import math

import jax
import jax.numpy as jnp
import numpy as np
from jax import lax
from jax.experimental import pallas as pl
from jax.experimental.pallas import tpu as pltpu
from jax.sharding import PartitionSpec as P

BZ = 64
SWEEPS = 8
LANES = 128
ROWS = 16
CHUNKS = 32
HALO = SWEEPS - 1
PAD = 10
SHELL = 8


def passed_along(x, axis, by):
    size = lax.axis_size(axis)
    pairs = [(i, i + by) for i in range(size) if 0 <= i + by < size]
    return lax.ppermute(x, axis, pairs)


def even_coefficients():
    nodes = np.polynomial.chebyshev.Chebyshev.basis(SWEEPS).convert(kind=np.polynomial.Polynomial)
    top = nodes.coef / 6.0 ** np.arange(SWEEPS + 1)
    rest = -top / float(nodes(6.5 / 6.0))
    rest[0] += 1.0
    even = rest[::2]
    g = np.zeros(SWEEPS // 2)
    carry = 0.0
    for k in range(SWEEPS // 2):
        g[k] = (even[k] + carry) / 42.25
        carry = g[k]
    return g


def slot_scalars(slot, right_ref, live_ref, c0_ref, c1_ref, c2_ref):
    right = right_ref[slot]
    row = right % 2
    step = right // 2
    left = slot % 2

    def corner(dim):
        near = c0_ref[row, dim].astype(jnp.float32)
        far = jnp.where(step == 1, c1_ref[row, dim], c2_ref[row, dim])
        return jnp.where(step == 0, near, far).astype(jnp.int32) - c0_ref[left, dim]

    return left, right, row, step, live_ref[slot], corner(0), corner(1)


def shift_parts(shift_y, shift_z):
    shift = shift_y * BZ + shift_z
    whole = shift >> 7
    part = shift & (LANES - 1)
    lane = lax.broadcasted_iota(jnp.int32, (ROWS, LANES), 1)
    source = (lane & (BZ - 1)) - shift_z
    keep = (source >= 0) & (source < BZ)
    return whole, part, keep & (lane >= part), keep & (lane < part)


def lanes_of(t):
    return pl.ds(t * LANES, LANES)


def density_kernel(right_ref, live_ref, c0_ref, c1_ref, c2_ref, own_ref, near_ref, far_ref,
                   moved_ref, up_ref, down_ref, rolled):
    rolled[...] = jnp.zeros_like(rolled)

    def one_slot(slot, _):
        left, right, row, step, live, dy, dz = slot_scalars(
            slot, right_ref, live_ref, c0_ref, c1_ref, c2_ref)
        whole, part, first, second = shift_parts(dy, dz)
        for k, source in enumerate((own_ref, near_ref, far_ref)):
            @pl.when(step == k)
            def _():
                for t in range(CHUNKS):
                    rolled[PAD + t] = pltpu.roll(source[row, :, lanes_of(t)], part, 1)
        scale = live.astype(jnp.float32)
        for t in range(CHUNKS):
            at = PAD + t - whole
            moved = jnp.where(first, rolled[at], jnp.where(second, rolled[at - 1], 0.0))
            moved_ref[slot, t] = moved
            density = own_ref[left, :, lanes_of(t)] * moved * scale
            up_ref[slot, HALO * t : HALO * (t + 1), :] = density[ROWS - HALO :]
            down_ref[slot, HALO * t : HALO * (t + 1), :] = density[:HALO]
        return 0

    lax.fori_loop(0, right_ref.shape[0], one_slot, 0)


def solve_kernel(coef, right_ref, live_ref, edge_ref, c0_ref, c1_ref, c2_ref, own_ref, moved_ref,
                 low_ref, high_ref, self_ref, near_ref, far_ref, dens, ping, pong, rolled):
    full = 4 * SHELL
    lane = lax.broadcasted_iota(jnp.int32, (full, LANES), 1)
    at_row = lax.broadcasted_iota(jnp.int32, (full, LANES), 0)
    lower_half = lane < BZ
    zpos = lane & (BZ - 1)
    has_lower = zpos > 0
    has_upper = zpos < BZ - 1
    keep_low = edge_ref[0]
    keep_high = edge_ref[1]
    inside = jnp.where(at_row < SHELL, keep_low, jnp.where(at_row >= 3 * SHELL, keep_high, 1.0))

    for field in (dens, ping, pong, rolled):
        field[...] = jnp.zeros_like(field)
    for out in (self_ref, near_ref, far_ref):
        out[...] = jnp.zeros_like(out)

    def neighbours(field, t, lo, hi):
        n = hi - lo
        here = field[t + 1, lo:hi, :]
        turned = [pltpu.roll(field[t + 1 + d, lo:hi, :], BZ, 1) for d in (-1, 0, 1)]
        total = field[t + 1, lo - 1 : hi - 1, :] + field[t + 1, lo + 1 : hi + 1, :]
        total = total + (turned[1] + jnp.where(lower_half[:n], turned[0], turned[2]))
        below = jnp.where(has_lower[:n], pltpu.roll(here, 1, 1), 0.0)
        above = jnp.where(has_upper[:n], pltpu.roll(here, LANES - 1, 1), 0.0)
        return here, total + (below + above)

    lo, hi = SHELL, SHELL + full

    def sweep(source, target, weight):
        for t in range(CHUNKS):
            _, total = neighbours(source, t, lo, hi)
            if weight is not None:
                total = total + weight * dens[t + 1, lo:hi, :]
            target[t + 1, lo:hi, :] = total * inside

    def one_slot(slot, _):
        left, right, row, step, live, dy, dz = slot_scalars(
            slot, right_ref, live_ref, c0_ref, c1_ref, c2_ref)
        scale = live.astype(jnp.float32)
        for t in range(CHUNKS):
            dens[t + 1, 2 * SHELL : 4 * SHELL, :] = (
                own_ref[left, :, lanes_of(t)] * moved_ref[slot, t] * scale)
            dens[t + 1, 2 * SHELL - HALO : 2 * SHELL, :] = low_ref[slot, HALO * t : HALO * (t + 1), :]
            dens[t + 1, 4 * SHELL : 4 * SHELL + HALO, :] = high_ref[slot, HALO * t : HALO * (t + 1), :]
        sweep(dens, ping, None)
        sweep(ping, pong, coef[2] / coef[3])
        sweep(pong, ping, None)
        sweep(ping, pong, coef[1] / coef[3])
        sweep(pong, ping, None)
        sweep(ping, pong, coef[0] / coef[3])
        whole, part, first, second = shift_parts(-dy, -dz)
        for t in range(CHUNKS):
            here, total = neighbours(pong, t, 2 * SHELL, 4 * SHELL)
            potential = (total + 6.5 * here) * coef[3]
            self_ref[left, :, lanes_of(t)] += potential * moved_ref[slot, t]
            rolled[PAD + t] = pltpu.roll(potential * own_ref[left, :, lanes_of(t)], part, 1)
        for k, target in enumerate((self_ref, near_ref, far_ref)):
            @pl.when(step == k)
            def _():
                for t in range(CHUNKS):
                    at = PAD + t - whole
                    target[row, :, lanes_of(t)] += jnp.where(
                        first, rolled[at], jnp.where(second, rolled[at - 1], 0.0))
        return 0

    lax.fori_loop(0, right_ref.shape[0], one_slot, 0)


def per_device(orbitals, corners, pair_partner, pair_live):
    per_owner, rows, flat = orbitals.shape
    slots = pair_partner.shape[0]
    base = lax.axis_index("wide") * per_owner
    place = lax.axis_index("quad")
    last = lax.axis_size("quad") - 1
    corner_float = corners.astype(jnp.float32)
    near_corner = passed_along(corner_float, "wide", -1)
    far_corner = passed_along(corner_float, "wide", -2)
    near = passed_along(orbitals, "wide", -1)
    far = passed_along(orbitals, "wide", -2)
    right = jnp.clip(pair_partner - base, 0, 3 * per_owner - 1)
    edge = jnp.stack([place > 0, place < last]).astype(jnp.float32)

    smem = pl.BlockSpec(memory_space=pltpu.SMEM)
    vmem = pl.BlockSpec(memory_space=pltpu.VMEM)
    f32 = jnp.float32
    box = jax.ShapeDtypeStruct((per_owner, rows, flat), f32)
    halo = jax.ShapeDtypeStruct((slots, HALO * CHUNKS, LANES), f32)
    moved, up, down = pl.pallas_call(
        density_kernel,
        out_shape=(jax.ShapeDtypeStruct((slots, CHUNKS, ROWS, LANES), f32), halo, halo),
        in_specs=[smem] * 5 + [vmem] * 3,
        out_specs=(vmem,) * 3,
        scratch_shapes=[pltpu.VMEM((CHUNKS + 2 * PAD, ROWS, LANES), f32)],
        cost_estimate=pl.CostEstimate(flops=4_000_000, bytes_accessed=4 << 20, transcendentals=0),
        name="density",
    )(right, pair_live, corners, near_corner, far_corner, orbitals, near, far)
    low = passed_along(up, "quad", 1)
    high = passed_along(down, "quad", -1)
    field = pltpu.VMEM((CHUNKS + 2, 6 * SHELL, LANES), f32)
    mine, to_near, to_far = pl.pallas_call(
        functools.partial(solve_kernel, [float(g) for g in even_coefficients()]),
        out_shape=(box,) * 3,
        in_specs=[smem] * 6 + [vmem] * 4,
        out_specs=(vmem,) * 3,
        scratch_shapes=[field] * 3 + [pltpu.VMEM((CHUNKS + 2 * PAD, ROWS, LANES), f32)],
        cost_estimate=pl.CostEstimate(flops=60_000_000, bytes_accessed=5 << 20, transcendentals=0),
        name="solve",
    )(right, pair_live, edge, corners, near_corner, far_corner, orbitals, moved, low, high)
    from_near = passed_along(to_near, "wide", 1)
    from_far = passed_along(to_far, "wide", 2)
    return mine + from_near + from_far


def solution(mesh):
    in_specs = (P("wide", "quad", None), P("wide", None), P("wide"), P("wide"))
    out_specs = P("wide", "quad", None)
    return jax.shard_map(
        per_device, mesh=mesh, in_specs=in_specs, out_specs=out_specs, check_vma=False
    )
```

```python
import functools
import math

import jax
import jax.numpy as jnp
import numpy as np
from jax import lax
from jax.experimental import pallas as pl
from jax.experimental.pallas import tpu as pltpu
from jax.sharding import PartitionSpec as P


BZ = 64
SWEEPS = 8
LANES = 128
ROWS = 16
CHUNKS = 32
HALO = SWEEPS - 1
PAD = 10
SHELL = 8


def passed_along(x, axis, by):
    size = lax.axis_size(axis)
    pairs = [(i, i + by) for i in range(size) if 0 <= i + by < size]
    return lax.ppermute(x, axis, pairs)


def even_coefficients():
    nodes = np.polynomial.chebyshev.Chebyshev.basis(SWEEPS).convert(kind=np.polynomial.Polynomial)
    top = nodes.coef / 6.0 ** np.arange(SWEEPS + 1)
    rest = -top / float(nodes(6.5 / 6.0))
    rest[0] += 1.0
    even = rest[::2]
    g = np.zeros(SWEEPS // 2)
    carry = 0.0
    for k in range(SWEEPS // 2):
        g[k] = (even[k] + carry) / 42.25
        carry = g[k]
    return g


def slot_scalars(slot, base_ref, meta_ref, own_ref, fore_ref):
    right = jnp.clip(meta_ref[4 + slot].astype(jnp.int32) - base_ref[0], 0, 5)
    row = right % 2
    step = right // 2
    left = slot % 2

    def offset(dim):
        at = 2 * row + dim
        near = jnp.where(step == 1, own_ref[at], fore_ref[at])
        there = jnp.where(step == 0, meta_ref[at], near)
        return (there - meta_ref[2 * left + dim]).astype(jnp.int32)

    return left, row, step, meta_ref[8 + slot], offset(0), offset(1)


def shift_parts(shift_y, shift_z, rows):
    shift = shift_y * BZ + shift_z
    whole = shift >> 7
    part = shift & (LANES - 1)
    lane = lax.broadcasted_iota(jnp.int32, (rows, LANES), 1)
    source = (lane & (BZ - 1)) - shift_z
    keep = (source >= 0) & (source < BZ)
    return whole, part, keep & (lane >= part), keep & (lane < part)


def lanes_of(t):
    return pl.ds(t * LANES, LANES)


def lane_table():
    lane = np.arange(LANES)
    half, zpos = lane // BZ, lane % BZ
    along_z = (half[:, None] == half[None, :]) & (np.abs(zpos[:, None] - zpos[None, :]) == 1)
    turned = (half[:, None] != half[None, :]) & (zpos[:, None] == zpos[None, :])
    table = np.concatenate([along_z | turned, turned], axis=1)
    return np.concatenate([table, table], axis=0).astype(np.float32)


FULL = 4 * SHELL
BANDS = ((0, SHELL), (SHELL, 3 * SHELL), (3 * SHELL, FULL))


def exchange_kernel(coef, slots, base_ref, meta_ref, own_corner_ref, fore_corner_ref, edge_ref,
                    back_low, back_mid, back_high, mine_low, mine_mid, mine_high,
                    fore_low, fore_mid, fore_high, table_ref, to_back, to_mine, to_fore,
                    rolled, moved_ref, dens, field, parts, sums):
    lower_half = lax.broadcasted_iota(jnp.int32, (FULL, LANES), 1) < BZ
    at_row = lax.broadcasted_iota(jnp.int32, (FULL, LANES), 0)
    inside = jnp.where(at_row < SHELL, edge_ref[0], jnp.where(at_row >= 3 * SHELL, edge_ref[1], 1.0))
    pool = ((back_low, back_mid, back_high), (mine_low, mine_mid, mine_high),
            (fore_low, fore_mid, fore_high))

    for end in (0, PAD + CHUNKS):
        rolled[end : end + PAD] = jnp.zeros((PAD, FULL, LANES), jnp.float32)
    for out in (to_back, to_mine, to_fore):
        out[...] = jnp.zeros_like(out)

    def cut(slot, t, value):
        high = value.astype(jnp.bfloat16)
        parts[slot, FULL * t : FULL * (t + 1), :LANES] = high
        parts[slot, FULL * t : FULL * (t + 1), LANES:] = (
            value - high.astype(jnp.float32)).astype(jnp.bfloat16)

    def multiply(slot):
        sums[slot, FULL : FULL * (CHUNKS + 1), :] = jnp.dot(
            parts[slot], table_ref[...], preferred_element_type=jnp.float32)

    def turned(slot, t, lo, hi):
        return sums[slot, FULL * (t + 1) + lo : FULL * (t + 1) + hi, LANES:]

    def neighbours(slot, lo, hi):
        before, here = turned(slot, -1, lo, hi), turned(slot, 0, lo, hi)
        at, n = SHELL + lo, hi - lo
        for t in range(CHUNKS):
            after = turned(slot, t + 1, lo, hi)
            total = field[slot, t, at - 1 : at - 1 + n, :] + field[slot, t, at + 1 : at + 1 + n, :]
            total = total + sums[slot, FULL * (t + 1) + lo : FULL * (t + 1) + hi, :LANES]
            yield t, total + jnp.where(lower_half[:n], before, after)
            before, here = here, after

    def sweep(slot, weight):
        for t, total in neighbours(slot, 0, FULL):
            if weight is not None:
                total = total + weight * dens[slot, t]
            total = total * inside
            field[slot, t, SHELL : SHELL + FULL, :] = total
            cut(slot, t, total)
        multiply(slot)

    def pair_density(slot, _):
        left, row, step, live, dy, dz = slot_scalars(
            slot, base_ref, meta_ref, own_corner_ref, fore_corner_ref)
        whole, part, first, second = shift_parts(dy, dz, FULL)
        for k, sources in enumerate(pool):
            @pl.when(step == k)
            def _():
                for t in range(CHUNKS):
                    for (lo, hi), source in zip(BANDS, sources):
                        rolled[PAD + t, lo:hi, :] = pltpu.roll(source[row, :, lanes_of(t)], part, 1)
        for end in (0, FULL * (CHUNKS + 1)):
            sums[slot, end : end + FULL, :] = jnp.zeros((FULL, 2 * LANES), jnp.float32)
        rim = jnp.zeros((SHELL, LANES), jnp.float32)
        for t in range(CHUNKS):
            at = PAD + t - whole
            moved = jnp.where(first, rolled[at], jnp.where(second, rolled[at - 1], 0.0))
            moved_ref[slot, t] = moved[SHELL : SHELL + ROWS]
            field[slot, t, :SHELL, :] = rim
            field[slot, t, SHELL + FULL :, :] = rim
            for (lo, hi), source in zip(BANDS, pool[0]):
                value = source[left, :, lanes_of(t)] * moved[lo:hi] * live
                dens[slot, t, lo:hi, :] = value
                field[slot, t, SHELL + lo : SHELL + hi, :] = value
            cut(slot, t, dens[slot, t])
        multiply(slot)
        return 0

    lax.fori_loop(0, slots, pair_density, 0)

    def two_sweeps(k, _):
        weight = jnp.where(k == 0, coef[2] / coef[3], jnp.where(k == 1, coef[1] / coef[3], coef[0] / coef[3]))
        for slot in range(slots):
            sweep(slot, None)
        for slot in range(slots):
            sweep(slot, weight)
        return 0

    lax.fori_loop(0, SWEEPS // 2 - 1, two_sweeps, 0)

    def terms(slot, _):
        left, row, step, live, dy, dz = slot_scalars(
            slot, base_ref, meta_ref, own_corner_ref, fore_corner_ref)
        whole, part, first, second = shift_parts(-dy, -dz, ROWS)
        for t, total in neighbours(slot, SHELL, SHELL + ROWS):
            here = field[slot, t, 2 * SHELL : 2 * SHELL + ROWS, :]
            potential = (total + 6.5 * here) * coef[3]
            to_back[left, :, lanes_of(t)] += potential * moved_ref[slot, t]
            rolled[PAD + t, :ROWS, :] = pltpu.roll(potential * back_mid[left, :, lanes_of(t)], part, 1)
        for k, target in enumerate((to_back, to_mine, to_fore)):
            @pl.when(step == k)
            def _():
                for t in range(CHUNKS):
                    at = PAD + t - whole
                    target[row, :, lanes_of(t)] += jnp.where(
                        first, rolled[at, :ROWS, :], jnp.where(second, rolled[at - 1, :ROWS, :], 0.0))
        return 0

    lax.fori_loop(0, slots, terms, 0)


def round_the_ring(x, axis, by):
    size = lax.axis_size(axis)
    return lax.ppermute(x, axis, [(i, (i + by) % size) for i in range(size)])


def per_device(orbitals, corners, pair_partner, pair_live):
    per_owner, rows, flat = orbitals.shape
    slots = pair_partner.shape[0]
    owners = lax.axis_size("wide")
    base = (lax.axis_index("wide") + owners - 1) % owners * per_owner
    place = lax.axis_index("quad")
    last = lax.axis_size("quad") - 1
    f32 = jnp.float32
    low = passed_along(orbitals[:, SHELL:, :], "quad", 1)
    high = passed_along(orbitals[:, :SHELL, :], "quad", -1)
    back_mid = round_the_ring(orbitals, "wide", 1)
    fore_mid = round_the_ring(orbitals, "wide", -1)
    meta = jnp.concatenate([corners.reshape(-1), pair_partner, pair_live]).astype(f32)
    back_meta = round_the_ring(meta, "wide", 1)
    fore_meta = round_the_ring(meta, "wide", -1)
    back_low = round_the_ring(low, "wide", 1)
    fore_low = round_the_ring(low, "wide", -1)
    back_high = round_the_ring(high, "wide", 1)
    fore_high = round_the_ring(high, "wide", -1)
    edge = jnp.stack([place > 0, place < last]).astype(f32)

    smem = pl.BlockSpec(memory_space=pltpu.SMEM)
    vmem = pl.BlockSpec(memory_space=pltpu.VMEM)
    box = jax.ShapeDtypeStruct((per_owner, rows, flat), f32)
    to_back, mine, to_fore = pl.pallas_call(
        functools.partial(exchange_kernel, [float(g) for g in even_coefficients()], slots),
        out_shape=(box,) * 3,
        in_specs=[smem] * 5 + [vmem] * 10,
        out_specs=(vmem,) * 3,
        scratch_shapes=[
            pltpu.VMEM((CHUNKS + 2 * PAD, FULL, LANES), f32),
            pltpu.VMEM((slots, CHUNKS, ROWS, LANES), f32),
            pltpu.VMEM((slots, CHUNKS, FULL, LANES), f32),
            pltpu.VMEM((slots, CHUNKS, FULL + 2 * SHELL, LANES), f32),
            pltpu.VMEM((slots, FULL * CHUNKS, 2 * LANES), jnp.bfloat16),
            pltpu.VMEM((slots, FULL * (CHUNKS + 2), 2 * LANES), f32),
        ],
        cost_estimate=pl.CostEstimate(flops=60_000_000, bytes_accessed=5 << 20, transcendentals=0),
        compiler_params=pltpu.CompilerParams(vmem_limit_bytes=28 << 20),
        name="exchange",
    )(base.reshape(1), back_meta, meta, fore_meta, edge,
      back_low, back_mid, back_high, low, orbitals, high, fore_low, fore_mid, fore_high,
      jnp.asarray(lane_table(), jnp.bfloat16))
    from_fore = round_the_ring(to_back, "wide", -1)
    from_back = round_the_ring(to_fore, "wide", 1)
    return mine + from_fore + from_back


def solution(mesh):
    in_specs = (P("wide", "quad", None), P("wide", None), P("wide"), P("wide"))
    out_specs = P("wide", "quad", None)
    return jax.shard_map(
        per_device, mesh=mesh, in_specs=in_specs, out_specs=out_specs, check_vma=False
    )
```

```python
import functools

import jax
import jax.numpy as jnp
import numpy as np
from jax import lax
from jax.experimental import pallas as pl
from jax.experimental.pallas import tpu as pltpu
from jax.sharding import PartitionSpec as P


BZ = 64
SWEEPS = 8
LANES = 128
ROWS = 16
CHUNKS = 32
PAD = 10
SHELL = 8


def even_coefficients():
    nodes = np.polynomial.chebyshev.Chebyshev.basis(SWEEPS).convert(kind=np.polynomial.Polynomial)
    top = nodes.coef / 6.0 ** np.arange(SWEEPS + 1)
    rest = -top / float(nodes(6.5 / 6.0))
    rest[0] += 1.0
    even = rest[::2]
    g = np.zeros(SWEEPS // 2)
    carry = 0.0
    for k in range(SWEEPS // 2):
        g[k] = (even[k] + carry) / 42.25
        carry = g[k]
    return g


def slot_scalars(slot, place_ref, meta_refs):
    across, own, inside = meta_refs
    first_core = place_ref[1] == 1

    def back(k):
        return jnp.where(first_core, across[k], inside[k])

    right = jnp.clip(back(4 + slot).astype(jnp.int32) - place_ref[0], 0, 5)
    row = right % 2
    step = right // 2
    left = slot % 2

    def offset(dim):
        at = 2 * row + dim
        fore = jnp.where(first_core, inside[at], across[at])
        there = jnp.where(step == 0, back(at), jnp.where(step == 1, own[at], fore))
        return (there - back(2 * left + dim)).astype(jnp.int32)

    which = jnp.where(step < 2, step, jnp.where(first_core, 2, 3))
    return left, row, which, back(8 + slot), offset(0), offset(1)


def shift_parts(shift_y, shift_z, rows):
    shift = shift_y * BZ + shift_z
    whole = shift >> 7
    part = shift & (LANES - 1)
    lane = lax.broadcasted_iota(jnp.int32, (rows, LANES), 1)
    source = (lane & (BZ - 1)) - shift_z
    keep = (source >= 0) & (source < BZ)
    return whole, part, keep & (lane >= part), keep & (lane < part)


def lanes_of(t):
    return pl.ds(t * LANES, LANES)


def lane_table():
    lane = np.arange(LANES)
    half, zpos = lane // BZ, lane % BZ
    along_z = (half[:, None] == half[None, :]) & (np.abs(zpos[:, None] - zpos[None, :]) == 1)
    turned = (half[:, None] != half[None, :]) & (zpos[:, None] == zpos[None, :])
    table = np.concatenate([along_z | turned, turned], axis=1)
    return np.concatenate([table, table], axis=0).astype(np.float32)


FULL = 4 * SHELL


def exchange_kernel(coef, slots, place_ref, across_meta, own_meta, inside_meta, edge_ref,
                    mine_mid, mine_halo, across_mid, across_halo, inside_mid, inside_halo, table_ref,
                    to_across, to_mine, to_inside,
                    back, to_back, rolled, moved_ref, dens, field, parts, sums):
    lower_half = lax.broadcasted_iota(jnp.int32, (FULL, LANES), 1) < BZ
    at_row = lax.broadcasted_iota(jnp.int32, (FULL, LANES), 0)
    inside = jnp.where(at_row < SHELL, edge_ref[0], jnp.where(at_row >= 3 * SHELL, edge_ref[1], 1.0))
    metas = (across_meta, own_meta, inside_meta)
    first_core = place_ref[1]
    low_at = pl.multiple_of(place_ref[2] * SHELL, SHELL)
    high_at = pl.multiple_of((1 - place_ref[2]) * SHELL, SHELL)

    def bands(mid, halo):
        def of(orbital, t):
            return ((0, SHELL, halo[orbital, pl.ds(low_at, SHELL), lanes_of(t)]),
                    (SHELL, 3 * SHELL, mid[orbital, :, lanes_of(t)]),
                    (3 * SHELL, FULL, halo[orbital, pl.ds(high_at, SHELL), lanes_of(t)]))

        return of

    def banded(orbital, t):
        return ((0, FULL, back[orbital, t]),)

    from_inside, from_across = bands(inside_mid, inside_halo), bands(across_mid, across_halo)
    pool = (banded, bands(mine_mid, mine_halo), from_inside, from_across)

    for k, source in enumerate((from_inside, from_across)):
        @pl.when(first_core == k)
        def _():
            for orbital in range(2):
                for t in range(CHUNKS):
                    for lo, hi, value in source(orbital, t):
                        back[orbital, t, lo:hi, :] = value

    for end in (0, PAD + CHUNKS):
        rolled[end : end + PAD] = jnp.zeros((PAD, FULL, LANES), jnp.float32)
    for out in (to_back, to_mine, to_inside, to_across):
        out[...] = jnp.zeros_like(out)

    def cut(slot, t, value):
        high = value.astype(jnp.bfloat16)
        parts[slot, FULL * t : FULL * (t + 1), :LANES] = high
        parts[slot, FULL * t : FULL * (t + 1), LANES:] = (
            value - high.astype(jnp.float32)).astype(jnp.bfloat16)

    def multiply(slot):
        sums[slot, FULL : FULL * (CHUNKS + 1), :] = jnp.dot(
            parts[slot], table_ref[...], preferred_element_type=jnp.float32)

    def turned(slot, t, lo, hi):
        return sums[slot, FULL * (t + 1) + lo : FULL * (t + 1) + hi, LANES:]

    def neighbours(slot, lo, hi):
        before, here = turned(slot, -1, lo, hi), turned(slot, 0, lo, hi)
        at, n = SHELL + lo, hi - lo
        for t in range(CHUNKS):
            after = turned(slot, t + 1, lo, hi)
            total = field[slot, t, at - 1 : at - 1 + n, :] + field[slot, t, at + 1 : at + 1 + n, :]
            total = total + sums[slot, FULL * (t + 1) + lo : FULL * (t + 1) + hi, :LANES]
            yield t, total + jnp.where(lower_half[:n], before, after)
            before, here = here, after

    def sweep(slot, weight):
        for t, total in neighbours(slot, 0, FULL):
            if weight is not None:
                total = total + weight * dens[slot, t]
            total = total * inside
            field[slot, t, SHELL : SHELL + FULL, :] = total
            cut(slot, t, total)
        multiply(slot)

    def pair_density(slot, _):
        left, row, which, live, dy, dz = slot_scalars(slot, place_ref, metas)
        whole, part, first, second = shift_parts(dy, dz, FULL)
        for k, source in enumerate(pool):
            @pl.when(which == k)
            def _():
                for t in range(CHUNKS):
                    for lo, hi, value in source(row, t):
                        rolled[PAD + t, lo:hi, :] = pltpu.roll(value, part, 1)
        for end in (0, FULL * (CHUNKS + 1)):
            sums[slot, end : end + FULL, :] = jnp.zeros((FULL, 2 * LANES), jnp.float32)
        rim = jnp.zeros((SHELL, LANES), jnp.float32)
        for t in range(CHUNKS):
            at = PAD + t - whole
            moved = jnp.where(first, rolled[at], jnp.where(second, rolled[at - 1], 0.0))
            moved_ref[slot, t] = moved[SHELL : SHELL + ROWS]
            field[slot, t, :SHELL, :] = rim
            field[slot, t, SHELL + FULL :, :] = rim
            value = back[left, t] * moved * live
            dens[slot, t] = value
            field[slot, t, SHELL : SHELL + FULL, :] = value
            cut(slot, t, value)
        multiply(slot)
        return 0

    lax.fori_loop(0, slots, pair_density, 0)

    def two_sweeps(k, _):
        weight = jnp.where(k == 0, coef[2] / coef[3], jnp.where(k == 1, coef[1] / coef[3], coef[0] / coef[3]))
        for slot in range(slots):
            sweep(slot, None)
        for slot in range(slots):
            sweep(slot, weight)
        return 0

    lax.fori_loop(0, SWEEPS // 2 - 1, two_sweeps, 0)

    def terms(slot, _):
        left, row, which, _, dy, dz = slot_scalars(slot, place_ref, metas)
        whole, part, first, second = shift_parts(-dy, -dz, ROWS)
        for t, total in neighbours(slot, SHELL, SHELL + ROWS):
            here = field[slot, t, 2 * SHELL : 2 * SHELL + ROWS, :]
            potential = (total + 6.5 * here) * coef[3]
            to_back[left, :, lanes_of(t)] += potential * moved_ref[slot, t]
            rolled[PAD + t, :ROWS, :] = pltpu.roll(
                potential * back[left, t, SHELL : SHELL + ROWS, :], part, 1)
        for k, target in enumerate((to_back, to_mine, to_inside, to_across)):
            @pl.when(which == k)
            def _():
                for t in range(CHUNKS):
                    at = PAD + t - whole
                    target[row, :, lanes_of(t)] += jnp.where(
                        first, rolled[at, :ROWS, :], jnp.where(second, rolled[at - 1, :ROWS, :], 0.0))
        return 0

    lax.fori_loop(0, slots, terms, 0)

    for k, out in enumerate((to_inside, to_across)):
        @pl.when(first_core == k)
        def _():
            out[...] = to_back[...]


def swapped(x, axis, first, ring):
    size = lax.axis_size(axis)
    lower = [i for i in range(first, size, 2) if ring or i + 1 < size]
    pairs = [(i, (i + 1) % size) for i in lower]
    return lax.ppermute(x, axis, pairs + [(b, a) for a, b in pairs])


def across_chips(x):
    return swapped(x, "wide", 1, True)


def inside_chip(x):
    return swapped(x, "wide", 0, True)


def per_device(orbitals, corners, pair_partner, pair_live):
    per_owner, rows, flat = orbitals.shape
    slots = pair_partner.shape[0]
    owners = lax.axis_size("wide")
    owner = lax.axis_index("wide")
    place = lax.axis_index("quad")
    last = lax.axis_size("quad") - 1
    f32 = jnp.float32
    even = 1 - place % 2
    tiles = orbitals.reshape(per_owner, 2, SHELL, flat)
    outer = lax.dynamic_index_in_dim(tiles, even, 1, keepdims=False)
    inner = lax.dynamic_index_in_dim(tiles, 1 - even, 1, keepdims=False)
    meta = jnp.concatenate([corners.reshape(-1), pair_partner, pair_live]).astype(f32)
    halo_one = swapped(outer, "quad", 0, False)
    halo_two = swapped(inner, "quad", 1, False)
    across_meta, inside_meta = across_chips(meta), inside_chip(meta)
    across_mid, inside_mid = across_chips(orbitals), inside_chip(orbitals)
    halo = jnp.concatenate([halo_one, halo_two], axis=1)
    across_halo, inside_halo = across_chips(halo), inside_chip(halo)
    where = jnp.stack([(owner + owners - 1) % owners * per_owner, 1 - owner % 2, even])
    edge = jnp.stack([place > 0, place < last]).astype(f32)

    smem = pl.BlockSpec(memory_space=pltpu.SMEM)
    vmem = pl.BlockSpec(memory_space=pltpu.VMEM)
    box = jax.ShapeDtypeStruct((per_owner, rows, flat), f32)
    to_across, mine, to_inside = pl.pallas_call(
        functools.partial(exchange_kernel, [float(g) for g in even_coefficients()], slots),
        out_shape=(box,) * 3,
        in_specs=[smem] * 5 + [vmem] * 7,
        out_specs=(vmem,) * 3,
        scratch_shapes=[
            pltpu.VMEM((per_owner, CHUNKS, FULL, LANES), f32),
            pltpu.VMEM((per_owner, rows, flat), f32),
            pltpu.VMEM((CHUNKS + 2 * PAD, FULL, LANES), f32),
            pltpu.VMEM((slots, CHUNKS, ROWS, LANES), f32),
            pltpu.VMEM((slots, CHUNKS, FULL, LANES), f32),
            pltpu.VMEM((slots, CHUNKS, FULL + 2 * SHELL, LANES), f32),
            pltpu.VMEM((slots, FULL * CHUNKS, 2 * LANES), jnp.bfloat16),
            pltpu.VMEM((slots, FULL * (CHUNKS + 2), 2 * LANES), f32),
        ],
        compiler_params=pltpu.CompilerParams(vmem_limit_bytes=28 << 20),
        cost_estimate=pl.CostEstimate(flops=60_000_000, bytes_accessed=5 << 20, transcendentals=0),
        name="exchange",
    )(where, across_meta, meta, inside_meta, edge,
      orbitals, halo, across_mid, across_halo, inside_mid, inside_halo,
      jnp.asarray(lane_table(), jnp.bfloat16))
    return mine + across_chips(to_across) + inside_chip(to_inside)


def solution(mesh):
    in_specs = (P("wide", "quad", None), P("wide", None), P("wide"), P("wide"))
    out_specs = P("wide", "quad", None)
    return jax.shard_map(
        per_device, mesh=mesh, in_specs=in_specs, out_specs=out_specs, check_vma=False
    )
```

```python
import functools

import jax
import jax.numpy as jnp
import numpy as np
from jax import lax
from jax.experimental import pallas as pl
from jax.experimental.pallas import tpu as pltpu
from jax.sharding import PartitionSpec as P


BZ = 64
SWEEPS = 8
LANES = 128
ROWS = 16
CHUNKS = 32
PAD = 10
SHELL = 8


def even_coefficients():
    nodes = np.polynomial.chebyshev.Chebyshev.basis(SWEEPS).convert(kind=np.polynomial.Polynomial)
    top = nodes.coef / 6.0 ** np.arange(SWEEPS + 1)
    rest = -top / float(nodes(6.5 / 6.0))
    rest[0] += 1.0
    even = rest[::2]
    g = np.zeros(SWEEPS // 2)
    carry = 0.0
    for k in range(SWEEPS // 2):
        g[k] = (even[k] + carry) / 42.25
        carry = g[k]
    return g


def slot_scalars(slot, place_ref, meta_refs):
    across, own, inside = meta_refs
    first_core = place_ref[1] == 1

    def back(k):
        return jnp.where(first_core, across[k], inside[k])

    right = jnp.clip(back(4 + slot).astype(jnp.int32) - place_ref[0], 0, 5)
    row = right % 2
    step = right // 2
    left = slot % 2

    def offset(dim):
        at = 2 * row + dim
        fore = jnp.where(first_core, inside[at], across[at])
        there = jnp.where(step == 0, back(at), jnp.where(step == 1, own[at], fore))
        return (there - back(2 * left + dim)).astype(jnp.int32)

    which = jnp.where(step < 2, step, jnp.where(first_core, 2, 3))
    return left, row, which, back(8 + slot), offset(0), offset(1)


def shift_parts(shift_y, shift_z, rows):
    shift = shift_y * BZ + shift_z
    whole = shift >> 7
    part = shift & (LANES - 1)
    lane = lax.broadcasted_iota(jnp.int32, (rows, LANES), 1)
    source = (lane & (BZ - 1)) - shift_z
    keep = (source >= 0) & (source < BZ)
    return whole, part, keep & (lane >= part), keep & (lane < part)


def lanes_of(t):
    return pl.ds(t * LANES, LANES)


def lane_table():
    lane = np.arange(LANES)
    half, zpos = lane // BZ, lane % BZ
    along_z = (half[:, None] == half[None, :]) & (np.abs(zpos[:, None] - zpos[None, :]) == 1)
    turned = (half[:, None] != half[None, :]) & (zpos[:, None] == zpos[None, :])
    table = np.concatenate([along_z | turned, turned], axis=1)
    return np.concatenate([table, table], axis=0).astype(np.float32)


FULL = 4 * SHELL


def exchange_kernel(coef, slots, place_ref, across_meta, own_meta, inside_meta, edge_ref,
                    mine_all, across_mid, across_halo, inside_all, table_ref,
                    to_across, to_mine, to_inside,
                    back, to_back, rolled, moved_ref, dens, field, parts, sums):
    lower_half = lax.broadcasted_iota(jnp.int32, (FULL, LANES), 1) < BZ
    at_row = lax.broadcasted_iota(jnp.int32, (FULL, LANES), 0)
    inside = jnp.where(at_row < SHELL, edge_ref[0], jnp.where(at_row >= 3 * SHELL, edge_ref[1], 1.0))
    metas = (across_meta, own_meta, inside_meta)
    first_core = place_ref[1]
    even = place_ref[2]

    def bands(mid, mid_at, halo, apart):
        low_at = pl.multiple_of(even * apart, SHELL)
        high_at = pl.multiple_of((1 - even) * apart, SHELL)

        def of(orbital, t):
            return ((0, SHELL, halo[orbital, pl.ds(low_at, SHELL), lanes_of(t)]),
                    (SHELL, 3 * SHELL, mid[orbital, mid_at : mid_at + ROWS, lanes_of(t)]),
                    (3 * SHELL, FULL, halo[orbital, pl.ds(high_at, SHELL), lanes_of(t)]))

        return of

    def banded(orbital, t):
        return ((0, FULL, back[orbital, t]),)

    from_inside = bands(inside_all, SHELL, inside_all, 3 * SHELL)
    from_across = bands(across_mid, 0, across_halo, SHELL)
    pool = (banded, bands(mine_all, SHELL, mine_all, 3 * SHELL), from_inside, from_across)

    for k, source in enumerate((from_inside, from_across)):
        @pl.when(first_core == k)
        def _():
            for orbital in range(2):
                for t in range(CHUNKS):
                    for lo, hi, value in source(orbital, t):
                        back[orbital, t, lo:hi, :] = value

    for end in (0, PAD + CHUNKS):
        rolled[end : end + PAD] = jnp.zeros((PAD, FULL, LANES), jnp.float32)
    for out in (to_back, to_mine, to_inside, to_across):
        out[...] = jnp.zeros_like(out)

    def cut(slot, t, value):
        high = value.astype(jnp.bfloat16)
        parts[slot, FULL * t : FULL * (t + 1), :LANES] = high
        parts[slot, FULL * t : FULL * (t + 1), LANES:] = (
            value - high.astype(jnp.float32)).astype(jnp.bfloat16)

    def multiply(slot):
        sums[slot, FULL : FULL * (CHUNKS + 1), :] = jnp.dot(
            parts[slot], table_ref[...], preferred_element_type=jnp.float32)

    def turned(slot, t, lo, hi):
        return sums[slot, FULL * (t + 1) + lo : FULL * (t + 1) + hi, LANES:]

    def neighbours(slot, lo, hi):
        before, here = turned(slot, -1, lo, hi), turned(slot, 0, lo, hi)
        at, n = SHELL + lo, hi - lo
        for t in range(CHUNKS):
            after = turned(slot, t + 1, lo, hi)
            total = field[slot, t, at - 1 : at - 1 + n, :] + field[slot, t, at + 1 : at + 1 + n, :]
            total = total + sums[slot, FULL * (t + 1) + lo : FULL * (t + 1) + hi, :LANES]
            yield t, total + jnp.where(lower_half[:n], before, after)
            before, here = here, after

    def sweep(slot, weight):
        for t, total in neighbours(slot, 0, FULL):
            if weight is not None:
                total = total + weight * dens[slot, t]
            total = total * inside
            field[slot, t, SHELL : SHELL + FULL, :] = total
            cut(slot, t, total)
        multiply(slot)

    def pair_density(slot, _):
        left, row, which, live, dy, dz = slot_scalars(slot, place_ref, metas)
        whole, part, first, second = shift_parts(dy, dz, FULL)
        for k, source in enumerate(pool):
            @pl.when(which == k)
            def _():
                for t in range(CHUNKS):
                    for lo, hi, value in source(row, t):
                        rolled[PAD + t, lo:hi, :] = pltpu.roll(value, part, 1)
        for end in (0, FULL * (CHUNKS + 1)):
            sums[slot, end : end + FULL, :] = jnp.zeros((FULL, 2 * LANES), jnp.float32)
        rim = jnp.zeros((SHELL, LANES), jnp.float32)
        for t in range(CHUNKS):
            at = PAD + t - whole
            moved = jnp.where(first, rolled[at], jnp.where(second, rolled[at - 1], 0.0))
            moved_ref[slot, t] = moved[SHELL : SHELL + ROWS]
            field[slot, t, :SHELL, :] = rim
            field[slot, t, SHELL + FULL :, :] = rim
            value = back[left, t] * moved * live
            dens[slot, t] = value
            field[slot, t, SHELL : SHELL + FULL, :] = value
            cut(slot, t, value)
        multiply(slot)
        return 0

    lax.fori_loop(0, slots, pair_density, 0)

    def two_sweeps(k, _):
        weight = jnp.where(k == 0, coef[2] / coef[3], jnp.where(k == 1, coef[1] / coef[3], coef[0] / coef[3]))
        for slot in range(slots):
            sweep(slot, None)
        for slot in range(slots):
            sweep(slot, weight)
        return 0

    lax.fori_loop(0, SWEEPS // 2 - 1, two_sweeps, 0)

    def terms(slot, _):
        left, row, which, _, dy, dz = slot_scalars(slot, place_ref, metas)
        whole, part, first, second = shift_parts(-dy, -dz, ROWS)
        for t, total in neighbours(slot, SHELL, SHELL + ROWS):
            here = field[slot, t, 2 * SHELL : 2 * SHELL + ROWS, :]
            potential = (total + 6.5 * here) * coef[3]
            to_back[left, :, lanes_of(t)] += potential * moved_ref[slot, t]
            rolled[PAD + t, :ROWS, :] = pltpu.roll(
                potential * back[left, t, SHELL : SHELL + ROWS, :], part, 1)
        for k, target in enumerate((to_back, to_mine, to_inside, to_across)):
            @pl.when(which == k)
            def _():
                for t in range(CHUNKS):
                    at = PAD + t - whole
                    target[row, :, lanes_of(t)] += jnp.where(
                        first, rolled[at, :ROWS, :], jnp.where(second, rolled[at - 1, :ROWS, :], 0.0))
        return 0

    lax.fori_loop(0, slots, terms, 0)

    for k, out in enumerate((to_inside, to_across)):
        @pl.when(first_core == k)
        def _():
            out[...] = to_back[...]


def swapped(x, axis, first, ring):
    size = lax.axis_size(axis)
    lower = [i for i in range(first, size, 2) if ring or i + 1 < size]
    pairs = [(i, (i + 1) % size) for i in lower]
    return lax.ppermute(x, axis, pairs + [(b, a) for a, b in pairs])


def across_chips(x):
    return swapped(x, "wide", 1, True)


def inside_chip(x):
    return swapped(x, "wide", 0, True)


def per_device(orbitals, corners, pair_partner, pair_live):
    per_owner, rows, flat = orbitals.shape
    slots = pair_partner.shape[0]
    owners = lax.axis_size("wide")
    owner = lax.axis_index("wide")
    place = lax.axis_index("quad")
    last = lax.axis_size("quad") - 1
    f32 = jnp.float32
    even = 1 - place % 2
    tiles = orbitals.reshape(per_owner, 2, SHELL, flat)
    outer = lax.dynamic_index_in_dim(tiles, even, 1, keepdims=False)
    inner = lax.dynamic_index_in_dim(tiles, 1 - even, 1, keepdims=False)
    meta = jnp.concatenate([corners.reshape(-1), pair_partner, pair_live]).astype(f32)
    unused = (SHELL - 1) * (1 - even)
    outer = lax.dynamic_update_slice(outer, meta.reshape(1, 1, -1), (0, unused, 0))
    halo_one = swapped(outer, "quad", 0, False)
    halo_two = swapped(inner, "quad", 1, False)
    across_mid = across_chips(orbitals)
    across_halo = across_chips(jnp.concatenate([halo_one, halo_two], axis=1))
    mine_all = jnp.concatenate([halo_one, orbitals, halo_two], axis=1)
    inside_all = inside_chip(mine_all)

    def meta_of(halos):
        return lax.dynamic_slice(halos, (0, SHELL - 1 - unused, 0), (1, 1, meta.size)).reshape(-1)

    across_meta, inside_meta = meta_of(across_halo), meta_of(inside_all)
    where = jnp.stack([(owner + owners - 1) % owners * per_owner, 1 - owner % 2, even])
    edge = jnp.stack([place > 0, place < last]).astype(f32)

    smem = pl.BlockSpec(memory_space=pltpu.SMEM)
    vmem = pl.BlockSpec(memory_space=pltpu.VMEM)
    box = jax.ShapeDtypeStruct((per_owner, rows, flat), f32)
    to_across, mine, to_inside = pl.pallas_call(
        functools.partial(exchange_kernel, [float(g) for g in even_coefficients()], slots),
        out_shape=(box,) * 3,
        in_specs=[smem] * 5 + [vmem] * 5,
        out_specs=(vmem,) * 3,
        scratch_shapes=[
            pltpu.VMEM((per_owner, CHUNKS, FULL, LANES), f32),
            pltpu.VMEM((per_owner, rows, flat), f32),
            pltpu.VMEM((CHUNKS + 2 * PAD, FULL, LANES), f32),
            pltpu.VMEM((slots, CHUNKS, ROWS, LANES), f32),
            pltpu.VMEM((slots, CHUNKS, FULL, LANES), f32),
            pltpu.VMEM((slots, CHUNKS, FULL + 2 * SHELL, LANES), f32),
            pltpu.VMEM((slots, FULL * CHUNKS, 2 * LANES), jnp.bfloat16),
            pltpu.VMEM((slots, FULL * (CHUNKS + 2), 2 * LANES), f32),
        ],
        compiler_params=pltpu.CompilerParams(vmem_limit_bytes=28 << 20),
        cost_estimate=pl.CostEstimate(flops=60_000_000, bytes_accessed=5 << 20, transcendentals=0),
        name="exchange",
    )(where, across_meta, meta, inside_meta, edge,
      mine_all, across_mid, across_halo, inside_all,
      jnp.asarray(lane_table(), jnp.bfloat16))
    return mine + across_chips(to_across) + inside_chip(to_inside)


def solution(mesh):
    in_specs = (P("wide", "quad", None), P("wide", None), P("wide"), P("wide"))
    out_specs = P("wide", "quad", None)
    return jax.shard_map(
        per_device, mesh=mesh, in_specs=in_specs, out_specs=out_specs, check_vma=False
    )
```

```python
import functools

import jax
import jax.numpy as jnp
import numpy as np
from jax import lax
from jax.experimental import pallas as pl
from jax.experimental.pallas import tpu as pltpu
from jax.sharding import PartitionSpec as P


BZ = 64
SWEEPS = 8
LANES = 128
ROWS = 16
CHUNKS = 32
PAD = 10
SHELL = 8


def even_coefficients():
    nodes = np.polynomial.chebyshev.Chebyshev.basis(SWEEPS).convert(kind=np.polynomial.Polynomial)
    top = nodes.coef / 6.0 ** np.arange(SWEEPS + 1)
    rest = -top / float(nodes(6.5 / 6.0))
    rest[0] += 1.0
    even = rest[::2]
    g = np.zeros(SWEEPS // 2)
    carry = 0.0
    for k in range(SWEEPS // 2):
        g[k] = (even[k] + carry) / 42.25
        carry = g[k]
    return g


def slot_scalars(slot, place_ref, meta_refs):
    across, own, inside = meta_refs
    first_core = place_ref[1] == 1

    def back(k):
        return jnp.where(first_core, across[k], inside[k])

    right = jnp.clip(back(4 + slot).astype(jnp.int32) - place_ref[0], 0, 5)
    row = right % 2
    step = right // 2
    left = slot % 2

    def offset(dim):
        at = 2 * row + dim
        fore = jnp.where(first_core, inside[at], across[at])
        there = jnp.where(step == 0, back(at), jnp.where(step == 1, own[at], fore))
        return (there - back(2 * left + dim)).astype(jnp.int32)

    which = jnp.where(step < 2, step, jnp.where(first_core, 2, 3))
    return left, row, which, back(8 + slot), offset(0), offset(1)


def shift_parts(shift_y, shift_z, rows):
    shift = shift_y * BZ + shift_z
    whole = shift >> 7
    part = shift & (LANES - 1)
    lane = lax.broadcasted_iota(jnp.int32, (rows, LANES), 1)
    source = (lane & (BZ - 1)) - shift_z
    keep = (source >= 0) & (source < BZ)
    return whole, part, keep & (lane >= part), keep & (lane < part)


def lanes_of(t):
    return pl.ds(t * LANES, LANES)


def lane_table():
    lane = np.arange(LANES)
    half, zpos = lane // BZ, lane % BZ
    along_z = (half[:, None] == half[None, :]) & (np.abs(zpos[:, None] - zpos[None, :]) == 1)
    turned = (half[:, None] != half[None, :]) & (zpos[:, None] == zpos[None, :])
    table = np.concatenate([along_z | turned, turned], axis=1)
    return np.concatenate([table, table], axis=0).astype(np.float32)


FULL = 4 * SHELL


def exchange_kernel(coef, slots, place_ref, across_meta, own_meta, inside_meta, edge_ref,
                    mine_mid, mine_halo, across_mid, across_halo, inside_all, table_ref,
                    to_across, to_mine, to_inside,
                    back, to_back, rolled, moved_ref, dens, field, parts, sums):
    lower_half = lax.broadcasted_iota(jnp.int32, (FULL, LANES), 1) < BZ
    at_row = lax.broadcasted_iota(jnp.int32, (FULL, LANES), 0)
    inside = jnp.where(at_row < SHELL, edge_ref[0], jnp.where(at_row >= 3 * SHELL, edge_ref[1], 1.0))
    metas = (across_meta, own_meta, inside_meta)
    first_core = place_ref[1]
    even = place_ref[2]
    low_of, high_of = even, 1 - even

    def bands(halo, mid):
        def of(orbital, t):
            return ((0, SHELL, halo[low_of, orbital, :, lanes_of(t)]),
                    *mid(orbital, t),
                    (3 * SHELL, FULL, halo[high_of, orbital, :, lanes_of(t)]))

        return of

    def slab(mid):
        return lambda orbital, t: ((SHELL, 3 * SHELL, mid[orbital, :, lanes_of(t)]),)

    def last_tiles(orbital, t):
        return tuple(
            ((1 + k) * SHELL, (2 + k) * SHELL, inside_all[2 + k, orbital, :, lanes_of(t)]) for k in range(2))

    def banded(orbital, t):
        return ((0, FULL, back[orbital, t]),)

    from_inside = bands(inside_all, last_tiles)
    from_across = bands(across_halo, slab(across_mid))
    pool = (banded, bands(mine_halo, slab(mine_mid)), from_inside, from_across)

    for k, source in enumerate((from_inside, from_across)):
        @pl.when(first_core == k)
        def _():
            for orbital in range(2):
                for t in range(CHUNKS):
                    for lo, hi, value in source(orbital, t):
                        back[orbital, t, lo:hi, :] = value

    for end in (0, PAD + CHUNKS):
        rolled[end : end + PAD] = jnp.zeros((PAD, FULL, LANES), jnp.float32)
    for out in (to_back, to_mine, to_inside, to_across):
        out[...] = jnp.zeros_like(out)

    def cut(slot, t, value):
        high = value.astype(jnp.bfloat16)
        parts[slot, FULL * t : FULL * (t + 1), :LANES] = high
        parts[slot, FULL * t : FULL * (t + 1), LANES:] = (
            value - high.astype(jnp.float32)).astype(jnp.bfloat16)

    def multiply(slot):
        sums[slot, FULL : FULL * (CHUNKS + 1), :] = jnp.dot(
            parts[slot], table_ref[...], preferred_element_type=jnp.float32)

    def turned(slot, t, lo, hi):
        return sums[slot, FULL * (t + 1) + lo : FULL * (t + 1) + hi, LANES:]

    def neighbours(slot, lo, hi):
        before, here = turned(slot, -1, lo, hi), turned(slot, 0, lo, hi)
        at, n = SHELL + lo, hi - lo
        for t in range(CHUNKS):
            after = turned(slot, t + 1, lo, hi)
            total = field[slot, t, at - 1 : at - 1 + n, :] + field[slot, t, at + 1 : at + 1 + n, :]
            total = total + sums[slot, FULL * (t + 1) + lo : FULL * (t + 1) + hi, :LANES]
            yield t, total + jnp.where(lower_half[:n], before, after)
            before, here = here, after

    def sweep(slot, weight):
        for t, total in neighbours(slot, 0, FULL):
            if weight is not None:
                total = total + weight * dens[slot, t]
            total = total * inside
            field[slot, t, SHELL : SHELL + FULL, :] = total
            cut(slot, t, total)
        multiply(slot)

    def pair_density(slot, _):
        left, row, which, live, dy, dz = slot_scalars(slot, place_ref, metas)
        whole, part, first, second = shift_parts(dy, dz, FULL)
        for k, source in enumerate(pool):
            @pl.when(which == k)
            def _():
                for t in range(CHUNKS):
                    for lo, hi, value in source(row, t):
                        rolled[PAD + t, lo:hi, :] = pltpu.roll(value, part, 1)
        for end in (0, FULL * (CHUNKS + 1)):
            sums[slot, end : end + FULL, :] = jnp.zeros((FULL, 2 * LANES), jnp.float32)
        rim = jnp.zeros((SHELL, LANES), jnp.float32)
        for t in range(CHUNKS):
            at = PAD + t - whole
            moved = jnp.where(first, rolled[at], jnp.where(second, rolled[at - 1], 0.0))
            moved_ref[slot, t] = moved[SHELL : SHELL + ROWS]
            field[slot, t, :SHELL, :] = rim
            field[slot, t, SHELL + FULL :, :] = rim
            value = back[left, t] * moved * live
            dens[slot, t] = value
            field[slot, t, SHELL : SHELL + FULL, :] = value
            cut(slot, t, value)
        multiply(slot)
        return 0

    lax.fori_loop(0, slots, pair_density, 0)

    def two_sweeps(k, _):
        weight = jnp.where(k == 0, coef[2] / coef[3], jnp.where(k == 1, coef[1] / coef[3], coef[0] / coef[3]))
        for slot in range(slots):
            sweep(slot, None)
        for slot in range(slots):
            sweep(slot, weight)
        return 0

    lax.fori_loop(0, SWEEPS // 2 - 1, two_sweeps, 0)

    def terms(slot, _):
        left, row, which, _, dy, dz = slot_scalars(slot, place_ref, metas)
        whole, part, first, second = shift_parts(-dy, -dz, ROWS)
        for t, total in neighbours(slot, SHELL, SHELL + ROWS):
            here = field[slot, t, 2 * SHELL : 2 * SHELL + ROWS, :]
            potential = (total + 6.5 * here) * coef[3]
            to_back[left, :, lanes_of(t)] += potential * moved_ref[slot, t]
            rolled[PAD + t, :ROWS, :] = pltpu.roll(
                potential * back[left, t, SHELL : SHELL + ROWS, :], part, 1)
        for k, target in enumerate((to_back, to_mine, to_inside, to_across)):
            @pl.when(which == k)
            def _():
                for t in range(CHUNKS):
                    at = PAD + t - whole
                    target[row, :, lanes_of(t)] += jnp.where(
                        first, rolled[at, :ROWS, :], jnp.where(second, rolled[at - 1, :ROWS, :], 0.0))
        return 0

    lax.fori_loop(0, slots, terms, 0)

    for k, out in enumerate((to_inside, to_across)):
        @pl.when(first_core == k)
        def _():
            out[...] = to_back[...]


def swapped(x, axis, first, ring):
    size = lax.axis_size(axis)
    lower = [i for i in range(first, size, 2) if ring or i + 1 < size]
    pairs = [(i, (i + 1) % size) for i in lower]
    return lax.ppermute(x, axis, pairs + [(b, a) for a, b in pairs])


def across_chips(x):
    return swapped(x, "wide", 1, True)


def inside_chip(x):
    return swapped(x, "wide", 0, True)


def per_device(orbitals, corners, pair_partner, pair_live):
    per_owner, rows, flat = orbitals.shape
    slots = pair_partner.shape[0]
    owners = lax.axis_size("wide")
    owner = lax.axis_index("wide")
    place = lax.axis_index("quad")
    last = lax.axis_size("quad") - 1
    f32 = jnp.float32
    even = 1 - place % 2
    tiles = orbitals.reshape(per_owner, 2, SHELL, flat)
    outer = lax.dynamic_index_in_dim(tiles, even, 1, keepdims=False)
    inner = lax.dynamic_index_in_dim(tiles, 1 - even, 1, keepdims=False)
    meta = jnp.concatenate([corners.reshape(-1), pair_partner, pair_live]).astype(f32)
    unused = (SHELL - 1) * (1 - even)
    outer = lax.dynamic_update_slice(outer, meta.reshape(1, 1, -1), (0, unused, 0))
    halo_one = swapped(outer, "quad", 0, False)
    halo_two = swapped(inner, "quad", 1, False)
    across_mid = across_chips(orbitals)
    halo = jnp.stack([halo_one, halo_two])
    across_halo = across_chips(halo)
    mine_all = jnp.concatenate([halo, jnp.moveaxis(tiles, 1, 0)])
    inside_all = inside_chip(mine_all)

    def meta_of(halos):
        return lax.dynamic_slice(
            halos, (0, 0, SHELL - 1 - unused, 0), (1, 1, 1, meta.size)).reshape(-1)

    across_meta, inside_meta = meta_of(across_halo), meta_of(inside_all)
    where = jnp.stack([(owner + owners - 1) % owners * per_owner, 1 - owner % 2, even])
    edge = jnp.stack([place > 0, place < last]).astype(f32)

    smem = pl.BlockSpec(memory_space=pltpu.SMEM)
    vmem = pl.BlockSpec(memory_space=pltpu.VMEM)
    box = jax.ShapeDtypeStruct((per_owner, rows, flat), f32)
    to_across, mine, to_inside = pl.pallas_call(
        functools.partial(exchange_kernel, [float(g) for g in even_coefficients()], slots),
        out_shape=(box,) * 3,
        in_specs=[smem] * 5 + [vmem] * 6,
        out_specs=(vmem,) * 3,
        scratch_shapes=[
            pltpu.VMEM((per_owner, CHUNKS, FULL, LANES), f32),
            pltpu.VMEM((per_owner, rows, flat), f32),
            pltpu.VMEM((CHUNKS + 2 * PAD, FULL, LANES), f32),
            pltpu.VMEM((slots, CHUNKS, ROWS, LANES), f32),
            pltpu.VMEM((slots, CHUNKS, FULL, LANES), f32),
            pltpu.VMEM((slots, CHUNKS, FULL + 2 * SHELL, LANES), f32),
            pltpu.VMEM((slots, FULL * CHUNKS, 2 * LANES), jnp.bfloat16),
            pltpu.VMEM((slots, FULL * (CHUNKS + 2), 2 * LANES), f32),
        ],
        compiler_params=pltpu.CompilerParams(vmem_limit_bytes=28 << 20),
        cost_estimate=pl.CostEstimate(flops=60_000_000, bytes_accessed=5 << 20, transcendentals=0),
        name="exchange",
    )(where, across_meta, meta, inside_meta, edge,
      orbitals, halo, across_mid, across_halo, inside_all,
      jnp.asarray(lane_table(), jnp.bfloat16))
    return mine + across_chips(to_across) + inside_chip(to_inside)


def solution(mesh):
    in_specs = (P("wide", "quad", None), P("wide", None), P("wide"), P("wide"))
    out_specs = P("wide", "quad", None)
    return jax.shard_map(
        per_device, mesh=mesh, in_specs=in_specs, out_specs=out_specs, check_vma=False
    )
```

```python
import functools

import jax
import jax.numpy as jnp
import numpy as np
from jax import lax
from jax.experimental import pallas as pl
from jax.experimental.pallas import tpu as pltpu
from jax.sharding import PartitionSpec as P


BZ = 64
SWEEPS = 8
LANES = 128
ROWS = 16
CHUNKS = 32
PAD = 10
SHELL = 8


def even_coefficients():
    nodes = np.polynomial.chebyshev.Chebyshev.basis(SWEEPS).convert(kind=np.polynomial.Polynomial)
    top = nodes.coef / 6.0 ** np.arange(SWEEPS + 1)
    rest = -top / float(nodes(6.5 / 6.0))
    rest[0] += 1.0
    even = rest[::2]
    g = np.zeros(SWEEPS // 2)
    carry = 0.0
    for k in range(SWEEPS // 2):
        g[k] = (even[k] + carry) / 42.25
        carry = g[k]
    return g


def slot_scalars(slot, place_ref, meta_refs):
    across, own, inside = meta_refs
    first_core = place_ref[1] == 1

    def back(k):
        return jnp.where(first_core, across[k], inside[k])

    right = jnp.clip(back(4 + slot).astype(jnp.int32) - place_ref[0], 0, 5)
    row = right % 2
    step = right // 2
    left = slot % 2

    def offset(dim):
        at = 2 * row + dim
        fore = jnp.where(first_core, inside[at], across[at])
        there = jnp.where(step == 0, back(at), jnp.where(step == 1, own[at], fore))
        return (there - back(2 * left + dim)).astype(jnp.int32)

    which = jnp.where(step < 2, step, jnp.where(first_core, 2, 3))
    return left, row, which, back(8 + slot), offset(0), offset(1)


def shift_parts(shift_y, shift_z, rows):
    shift = shift_y * BZ + shift_z
    whole = shift >> 7
    part = shift & (LANES - 1)
    lane = lax.broadcasted_iota(jnp.int32, (rows, LANES), 1)
    source = (lane & (BZ - 1)) - shift_z
    keep = (source >= 0) & (source < BZ)
    return whole, part, keep & (lane >= part), keep & (lane < part)


def lanes_of(t):
    return pl.ds(t * LANES, LANES)


def lane_table():
    lane = np.arange(LANES)
    half, zpos = lane // BZ, lane % BZ
    along_z = (half[:, None] == half[None, :]) & (np.abs(zpos[:, None] - zpos[None, :]) == 1)
    turned = (half[:, None] != half[None, :]) & (zpos[:, None] == zpos[None, :])
    table = np.concatenate([along_z | turned, turned], axis=1)
    return np.concatenate([table, table], axis=0).astype(np.float32)


FULL = 4 * SHELL


def exchange_kernel(coef, slots, place_ref, across_meta, own_meta, inside_meta, edge_ref,
                    mine_mid, mine_halo, across_mid, across_halo, inside_all, table_ref,
                    to_across, to_mine, to_inside,
                    back, to_back, rolled, moved_ref, dens, field, parts, sums):
    lower_half = lax.broadcasted_iota(jnp.int32, (FULL, LANES), 1) < BZ
    at_row = lax.broadcasted_iota(jnp.int32, (FULL, LANES), 0)
    inside = jnp.where(at_row < SHELL, edge_ref[0], jnp.where(at_row >= 3 * SHELL, edge_ref[1], 1.0))
    metas = (across_meta, own_meta, inside_meta)
    first_core = place_ref[1]
    even = place_ref[2]
    low_of, high_of = even, 1 - even

    def bands(halo, mid):
        def of(orbital, t):
            return ((0, SHELL, halo[low_of, orbital, :, lanes_of(t)]),
                    *mid(orbital, t),
                    (3 * SHELL, FULL, halo[high_of, orbital, :, lanes_of(t)]))

        return of

    def slab(mid):
        return lambda orbital, t: ((SHELL, 3 * SHELL, mid[orbital, :, lanes_of(t)]),)

    def last_tiles(orbital, t):
        return tuple(
            ((1 + k) * SHELL, (2 + k) * SHELL, inside_all[2 + k, orbital, :, lanes_of(t)]) for k in range(2))

    def banded(orbital, t):
        return ((0, FULL, back[orbital, t]),)

    from_inside = bands(inside_all, last_tiles)
    from_across = bands(across_halo, slab(across_mid))
    pool = (banded, bands(mine_halo, slab(mine_mid)), from_inside, from_across)

    for k, source in enumerate((from_inside, from_across)):
        @pl.when(first_core == k)
        def _():
            for orbital in range(2):
                for t in range(CHUNKS):
                    for lo, hi, value in source(orbital, t):
                        back[orbital, t, lo:hi, :] = value

    for end in (0, PAD + CHUNKS):
        rolled[end : end + PAD] = jnp.zeros((PAD, FULL, LANES), jnp.float32)
    for out in (to_back, to_mine, to_inside, to_across):
        out[...] = jnp.zeros_like(out)

    def cut(slot, t, value):
        high = value.astype(jnp.bfloat16)
        parts[slot, FULL * t : FULL * (t + 1), :LANES] = high
        parts[slot, FULL * t : FULL * (t + 1), LANES:] = (
            value - high.astype(jnp.float32)).astype(jnp.bfloat16)

    def multiply(slot):
        sums[slot, FULL : FULL * (CHUNKS + 1), :] = jnp.dot(
            parts[slot], table_ref[...], preferred_element_type=jnp.float32)

    def turned(slot, t, lo, hi):
        return sums[slot, FULL * (t + 1) + lo : FULL * (t + 1) + hi, LANES:]

    def neighbours(slot, lo, hi):
        before, here = turned(slot, -1, lo, hi), turned(slot, 0, lo, hi)
        at, n = SHELL + lo, hi - lo
        for t in range(CHUNKS):
            after = turned(slot, t + 1, lo, hi)
            total = field[slot, t, at - 1 : at - 1 + n, :] + field[slot, t, at + 1 : at + 1 + n, :]
            total = total + sums[slot, FULL * (t + 1) + lo : FULL * (t + 1) + hi, :LANES]
            yield t, total + jnp.where(lower_half[:n], before, after)
            before, here = here, after

    def sweep(slot, weight):
        for t, total in neighbours(slot, 0, FULL):
            if weight is not None:
                total = total + weight * dens[slot, t]
            total = total * inside
            field[slot, t, SHELL : SHELL + FULL, :] = total
            cut(slot, t, total)
        multiply(slot)

    def pair_density(slot, _):
        left, row, which, live, dy, dz = slot_scalars(slot, place_ref, metas)
        whole, part, first, second = shift_parts(dy, dz, FULL)
        for k, source in enumerate(pool):
            @pl.when(which == k)
            def _():
                for t in range(CHUNKS):
                    for lo, hi, value in source(row, t):
                        rolled[PAD + t, lo:hi, :] = pltpu.roll(value, part, 1)
        for end in (0, FULL * (CHUNKS + 1)):
            sums[slot, end : end + FULL, :] = jnp.zeros((FULL, 2 * LANES), jnp.float32)
        rim = jnp.zeros((SHELL, LANES), jnp.float32)
        for t in range(CHUNKS):
            at = PAD + t - whole
            moved = jnp.where(first, rolled[at], jnp.where(second, rolled[at - 1], 0.0))
            moved_ref[slot, t] = moved[SHELL : SHELL + ROWS]
            field[slot, t, :SHELL, :] = rim
            field[slot, t, SHELL + FULL :, :] = rim
            value = back[left, t] * moved * live
            dens[slot, t] = value
            field[slot, t, SHELL : SHELL + FULL, :] = value
            cut(slot, t, value)
        multiply(slot)
        return 0

    lax.fori_loop(0, slots, pair_density, 0)

    for k in reversed(range(SWEEPS // 2 - 1)):
        for slot in range(slots):
            sweep(slot, None)
        for slot in range(slots):
            sweep(slot, coef[k] / coef[-1])

    def terms(slot, _):
        left, row, which, _, dy, dz = slot_scalars(slot, place_ref, metas)
        whole, part, first, second = shift_parts(-dy, -dz, ROWS)
        for t, total in neighbours(slot, SHELL, SHELL + ROWS):
            here = field[slot, t, 2 * SHELL : 2 * SHELL + ROWS, :]
            potential = (total + 6.5 * here) * coef[3]
            to_back[left, :, lanes_of(t)] += potential * moved_ref[slot, t]
            rolled[PAD + t, :ROWS, :] = pltpu.roll(
                potential * back[left, t, SHELL : SHELL + ROWS, :], part, 1)
        for k, target in enumerate((to_back, to_mine, to_inside, to_across)):
            @pl.when(which == k)
            def _():
                for t in range(CHUNKS):
                    at = PAD + t - whole
                    target[row, :, lanes_of(t)] += jnp.where(
                        first, rolled[at, :ROWS, :], jnp.where(second, rolled[at - 1, :ROWS, :], 0.0))
        return 0

    lax.fori_loop(0, slots, terms, 0)

    for k, out in enumerate((to_inside, to_across)):
        @pl.when(first_core == k)
        def _():
            out[...] = to_back[...]


def swapped(x, axis, first, ring):
    size = lax.axis_size(axis)
    lower = [i for i in range(first, size, 2) if ring or i + 1 < size]
    pairs = [(i, (i + 1) % size) for i in lower]
    return lax.ppermute(x, axis, pairs + [(b, a) for a, b in pairs])


def across_chips(x):
    return swapped(x, "wide", 1, True)


def inside_chip(x):
    return swapped(x, "wide", 0, True)


def per_device(orbitals, corners, pair_partner, pair_live):
    per_owner, rows, flat = orbitals.shape
    slots = pair_partner.shape[0]
    owners = lax.axis_size("wide")
    owner = lax.axis_index("wide")
    place = lax.axis_index("quad")
    last = lax.axis_size("quad") - 1
    f32 = jnp.float32
    even = 1 - place % 2
    tiles = orbitals.reshape(per_owner, 2, SHELL, flat)
    outer = lax.dynamic_index_in_dim(tiles, even, 1, keepdims=False)
    inner = lax.dynamic_index_in_dim(tiles, 1 - even, 1, keepdims=False)
    meta = jnp.concatenate([corners.reshape(-1), pair_partner, pair_live]).astype(f32)
    unused = (SHELL - 1) * (1 - even)
    outer = lax.dynamic_update_slice(outer, meta.reshape(1, 1, -1), (0, unused, 0))
    halo_one = swapped(outer, "quad", 0, False)
    halo_two = swapped(inner, "quad", 1, False)
    across_mid = across_chips(orbitals)
    halo = jnp.stack([halo_one, halo_two])
    across_halo = across_chips(halo)
    mine_all = jnp.concatenate([halo, jnp.moveaxis(tiles, 1, 0)])
    inside_all = inside_chip(mine_all)

    def meta_of(halos):
        return lax.dynamic_slice(
            halos, (0, 0, SHELL - 1 - unused, 0), (1, 1, 1, meta.size)).reshape(-1)

    across_meta, inside_meta = meta_of(across_halo), meta_of(inside_all)
    where = jnp.stack([(owner + owners - 1) % owners * per_owner, 1 - owner % 2, even])
    edge = jnp.stack([place > 0, place < last]).astype(f32)

    smem = pl.BlockSpec(memory_space=pltpu.SMEM)
    vmem = pl.BlockSpec(memory_space=pltpu.VMEM)
    box = jax.ShapeDtypeStruct((per_owner, rows, flat), f32)
    to_across, mine, to_inside = pl.pallas_call(
        functools.partial(exchange_kernel, [float(g) for g in even_coefficients()], slots),
        out_shape=(box,) * 3,
        in_specs=[smem] * 5 + [vmem] * 6,
        out_specs=(vmem,) * 3,
        scratch_shapes=[
            pltpu.VMEM((per_owner, CHUNKS, FULL, LANES), f32),
            pltpu.VMEM((per_owner, rows, flat), f32),
            pltpu.VMEM((CHUNKS + 2 * PAD, FULL, LANES), f32),
            pltpu.VMEM((slots, CHUNKS, ROWS, LANES), f32),
            pltpu.VMEM((slots, CHUNKS, FULL, LANES), f32),
            pltpu.VMEM((slots, CHUNKS, FULL + 2 * SHELL, LANES), f32),
            pltpu.VMEM((slots, FULL * CHUNKS, 2 * LANES), jnp.bfloat16),
            pltpu.VMEM((slots, FULL * (CHUNKS + 2), 2 * LANES), f32),
        ],
        compiler_params=pltpu.CompilerParams(vmem_limit_bytes=28 << 20),
        cost_estimate=pl.CostEstimate(flops=60_000_000, bytes_accessed=5 << 20, transcendentals=0),
        name="exchange",
    )(where, across_meta, meta, inside_meta, edge,
      orbitals, halo, across_mid, across_halo, inside_all,
      jnp.asarray(lane_table(), jnp.bfloat16))
    return mine + across_chips(to_across) + inside_chip(to_inside)


def solution(mesh):
    in_specs = (P("wide", "quad", None), P("wide", None), P("wide"), P("wide"))
    out_specs = P("wide", "quad", None)
    return jax.shard_map(
        per_device, mesh=mesh, in_specs=in_specs, out_specs=out_specs, check_vma=False
    )
```
